256 devices in a mesh: lon: 16 (over y_lo, z), lat: 16 (over y_hi, x, core).
Axes of the slice: x: 4, y: 4 (y_hi: 2, y_lo: 2; y = y_hi * 2 + y_lo), z: 8, core: 2. Of those that a mesh axis runs over, the one named last changes fastest.
Arguments:
- fields_in: bfloat16 [2, 192, 384, 512], P(None, 'lat', 'lon'), may hold values from -6 to 6
- level_map: int32 [2, 192, 384], P(None, 'lat', 'lon'), may hold values from 0 to 12
- land_sea: int32 [192, 384], P('lat', 'lon'), may hold values 0 or 1
- level_table: bfloat16 [13, 512], replicated, may hold values from -4 to 4
- surface_table: bfloat16 [2, 512], replicated, may hold values from -4 to 4
- norm_gain: bfloat16 [512], replicated, may hold values from 0.25 to 1.75
- w_qkv: bfloat16 [512, 1536], replicated, may hold values from -1 to 1
- w_proj: bfloat16 [512, 512], replicated, may hold values from -0.25 to 0.25
- merge_gain: bfloat16 [2048], replicated, may hold values from 0.25 to 1.75
- w_merge: bfloat16 [2048, 1024], replicated, may hold values from -0.125 to 0.125
- coarse_gain: bfloat16 [1024], replicated, may hold values from 0.25 to 1.75
- w_in: bfloat16 [1024, 4096], P(None, 'lat'), may hold values from -0.1875 to 0.1875
- w_out: bfloat16 [4096, 1024], P('lat'), may hold values from -0.09375 to 0.09375
- w_expand: bfloat16 [1024, 2048], replicated, may hold values from -0.1875 to 0.1875
- cotangent: bfloat16 [2, 192, 384, 512], P(None, 'lat', 'lon'), may hold values from -6 to 6
Outputs:
- fields_out: bfloat16 [2, 192, 384, 512], P(None, 'lat', 'lon')
- grad_in: float32 [1024, 4096], P('lon', 'lat')
- grad_out: float32 [4096, 1024], P('lat', 'lon')
The draws below stay inside these ranges and needn't reach their ends.
All inputs are finite; a program needn't handle non-finite values. No bound on the sum of `land_sea` on one device may be relied on, other than what follows from the above.
Results may differ from the reference program's by a relative error of at most 0.025.
Values may be sent and summed in bfloat16 or wider, within the bound.
No kernel may reach another device: no remote copies, remote signals or barrier semaphores. Data moves between devices by JAX's collectives and lax.ppermute only.
A program may use at most 128 MiB of HBM per device.

```python
import math
import jax
import jax.numpy as jnp
from jax import lax

C1 = 512
C2 = 1024
FF2 = 4096
HEADS = 8
NLEV = 13
LEVELS = 2
WIN_LAT = 12
WIN_LON = 6
SHIFT_LAT = 6
SHIFT_LON = 3
LAT = 192
LON = 384


def draw_w_qkv(key, part):
    first = jax.random.fold_in(key, 0)
    base = jax.random.normal(first, (C1, 3 * C1), jnp.float32) * C1 ** (-0.5)
    return jnp.clip(base, -1.0, 1.0).astype(jnp.bfloat16)


def with_ends(values, key, least, largest):
    longest = values.shape.index(max(values.shape))
    spots = []
    for shift in (0, 1):
        where = [jax.random.randint(jax.random.fold_in(key, axis), (), 0, length) for axis, length in enumerate(values.shape)]
        where[longest] = (where[longest] + shift) % values.shape[longest]
        spots.append(tuple(where))
    return values.at[spots[0]].set(least).at[spots[1]].set(largest)


def shard_levels(rng, extent, cuts, smallest, top_value):
    level = 1.0
    for axis_at, parts in cuts:
        heights = jax.random.uniform(jax.random.fold_in(jax.random.fold_in(rng, 6), axis_at), (parts,), jnp.float32, smallest / len(cuts), top_value / len(cuts))
        level = level * jnp.repeat(jnp.exp(heights), extent[axis_at] // parts).reshape((-1,) + (1,) * (len(extent) - 1 - axis_at))
    return level


def scatter_about(own_key, extent, scale, most, shards=(), kind=jnp.bfloat16):
    result = scale * jax.random.normal(own_key, extent, jnp.float32)
    if shards:
        result = result * shard_levels(own_key, extent, shards, -0.22, 0.18)
    return jnp.clip(result, -most, most).astype(kind)


def setup_inputs(seed: int = 0) -> dict:
    key_list = jax.random.split(jax.random.key(seed), 16)
    fields_in = scatter_about(key_list[0], (LEVELS, LAT, LON, C1), 1.0, 6.0, ((1, 16), (2, 16)))
    level_map = with_ends(jax.random.randint(key_list[1], (LEVELS, LAT, LON), 0, NLEV), jax.random.fold_in(key_list[1], 1), 0, NLEV - 1).astype(jnp.int32)
    land_sea = with_ends((jax.random.randint(key_list[2], (LAT, LON), 0, 3) < 1).astype(jnp.int32), jax.random.fold_in(key_list[2], 1), 0, 1)
    level_table = scatter_about(key_list[3], (NLEV, C1), 0.7, 4.0)
    surface_table = scatter_about(key_list[4], (2, C1), 0.7, 4.0)
    norm_gain = jnp.clip(1.0 + 0.15 * jax.random.normal(key_list[5], (C1,), jnp.float32), 0.25, 1.75).astype(jnp.bfloat16)
    w_qkv = draw_w_qkv(jax.random.fold_in(key_list[15], 71), 0)
    w_proj = scatter_about(key_list[7], (C1, C1), C1 ** -0.5, 0.25)
    merge_gain = jnp.clip(1.0 + 0.15 * jax.random.normal(key_list[8], (4 * C1,), jnp.float32), 0.25, 1.75).astype(jnp.bfloat16)
    w_merge = scatter_about(key_list[9], (4 * C1, C2), (4 * C1) ** -0.5, 0.125)
    coarse_gain = jnp.clip(1.0 + 0.15 * jax.random.normal(key_list[10], (C2,), jnp.float32), 0.25, 1.75).astype(jnp.bfloat16)
    w_in = scatter_about(key_list[11], (C2, FF2), C2 ** -0.5, 0.1875, ((1, 16),))
    w_out = scatter_about(key_list[12], (FF2, C2), FF2 ** -0.5, 0.09375, ((0, 16),))
    w_expand = scatter_about(key_list[13], (C2, 4 * C1), C2 ** -0.5, 0.1875)
    cotangent = scatter_about(key_list[14], (LEVELS, LAT, LON, C1), 1.0, 6.0, ((1, 16), (2, 16)))
    return {"fields_in": fields_in, "level_map": level_map, "land_sea": land_sea, "level_table": level_table, "surface_table": surface_table, "norm_gain": norm_gain, "w_qkv": w_qkv, "w_proj": w_proj, "merge_gain": merge_gain, "w_merge": w_merge, "coarse_gain": coarse_gain, "w_in": w_in, "w_out": w_out, "w_expand": w_expand, "cotangent": cotangent}


EPSILON = 1e-05

def layer_norm(values, gain):
    center = values - lax.optimization_barrier(jnp.mean(values, axis=-1, keepdims=True))
    spread = lax.optimization_barrier(jnp.mean(center * center, axis=-1, keepdims=True))
    return center * lax.rsqrt(spread + EPSILON) * gain.astype(jnp.float32)

def activate(values):
    return jax.nn.gelu(values, approximate=True)

def window_attention(packed, lat_index, lat_total):
    levels, rows, cols, triple = packed.shape
    width = triple // 3
    head_size = width // HEADS
    count_rows = rows // WIN_LAT
    count_cols = cols // WIN_LON
    window = levels * WIN_LAT * WIN_LON
    blocks = packed.reshape(levels, count_rows, WIN_LAT, count_cols, WIN_LON, triple)
    blocks = blocks.transpose(1, 3, 0, 2, 4, 5).reshape(count_rows * count_cols, window, triple)
    blocks = blocks.astype(jnp.float32)
    queries = blocks[:, :, :width].reshape(-1, window, HEADS, head_size)
    keys = blocks[:, :, width:2 * width].reshape(-1, window, HEADS, head_size)
    values = blocks[:, :, 2 * width:].reshape(-1, window, HEADS, head_size)
    scores = jnp.einsum('wqhd,wkhd->whqk', queries, keys) * (1.0 / math.sqrt(head_size))
    token_row = jnp.arange(window, dtype=jnp.int32) // WIN_LON % WIN_LAT
    block_row = jnp.arange(count_rows * count_cols, dtype=jnp.int32) // count_cols
    global_row = lat_index * rows + block_row[:, None] * WIN_LAT + token_row[None, :]
    region = (global_row >= lat_total - WIN_LAT).astype(jnp.int32) + (global_row >= lat_total - SHIFT_LAT).astype(jnp.int32)
    same = region[:, :, None] == region[:, None, :]
    scores = jnp.where(same[:, None], scores, -1e+30)
    top = lax.optimization_barrier(jnp.max(scores, axis=-1, keepdims=True))
    expos = jnp.exp(scores - top)
    probs = (expos / lax.optimization_barrier(jnp.sum(expos, axis=-1, keepdims=True))).astype(jnp.bfloat16)
    mixed = jnp.einsum('whqk,wkhd->wqhd', probs.astype(jnp.float32), values).astype(jnp.bfloat16)
    mixed = mixed.reshape(count_rows, count_cols, levels, WIN_LAT, WIN_LON, width)
    return mixed.transpose(2, 0, 3, 1, 4, 5).reshape(levels, rows, cols, width)

def merge_tokens(grid):
    levels, rows, cols, width = grid.shape
    blocks = grid.reshape(levels, rows // 2, 2, cols // 2, 2, width).transpose(0, 1, 3, 4, 2, 5)
    return blocks.reshape(-1, 4 * width)

def split_tokens(tokens, levels, rows, cols):
    width = tokens.shape[-1] // 4
    blocks = tokens.reshape(levels, rows // 2, cols // 2, 2, 2, width).transpose(0, 1, 4, 2, 3, 5)
    return blocks.reshape(levels, rows, cols, width)

def reference(fields_in, level_map, land_sea, level_table, surface_table, norm_gain, w_qkv, w_proj, merge_gain, w_merge, coarse_gain, w_in, w_out, w_expand, cotangent):
    width = fields_in.shape[-1]
    level_bias = level_table.astype(jnp.float32)[level_map]
    surface_bias = jnp.where(land_sea[..., None] == 1, surface_table[1].astype(jnp.float32), surface_table[0].astype(jnp.float32))
    fields = fields_in.astype(jnp.float32) + level_bias + surface_bias[None]
    normed = layer_norm(fields, norm_gain).astype(jnp.bfloat16)
    packed = jnp.dot(normed.reshape(-1, width), w_qkv, preferred_element_type=jnp.float32).astype(jnp.bfloat16)
    packed = packed.reshape(LEVELS, LAT, LON, 3 * width)
    rolled = jnp.roll(packed, (-SHIFT_LAT, -SHIFT_LON), axis=(1, 2))
    stacked = rolled.reshape(LEVELS, LAT // WIN_LAT, WIN_LAT, LON, 3 * width).transpose(1, 0, 2, 3, 4)
    index_rows = jnp.arange(LAT // WIN_LAT, dtype=jnp.int32)
    attended = lax.map(lambda pair: window_attention(pair[0], pair[1], LAT), (stacked, index_rows))
    attended = attended.transpose(1, 0, 2, 3, 4).reshape(LEVELS, LAT, LON, width)
    attended = jnp.roll(attended, (SHIFT_LAT, SHIFT_LON), axis=(1, 2))
    projected = jnp.dot(attended.reshape(-1, width), w_proj, preferred_element_type=jnp.float32)
    skip = (fields + projected.reshape(fields.shape)).astype(jnp.bfloat16)
    merged_normed = layer_norm(merge_tokens(skip).astype(jnp.float32), merge_gain).astype(jnp.bfloat16)
    coarse = jnp.dot(merged_normed, w_merge, preferred_element_type=jnp.float32).astype(jnp.bfloat16)
    coarse_normed = layer_norm(coarse.astype(jnp.float32), coarse_gain).astype(jnp.bfloat16)
    act = jnp.dot(coarse_normed, w_in, preferred_element_type=jnp.float32)
    hidden = activate(act).astype(jnp.bfloat16)
    coarse_out = (coarse.astype(jnp.float32) + jnp.dot(hidden, w_out, preferred_element_type=jnp.float32)).astype(jnp.bfloat16)
    expanded = jnp.dot(coarse_out, w_expand, preferred_element_type=jnp.float32)
    fields_out = (skip.astype(jnp.float32) + split_tokens(expanded, LEVELS, LAT, LON)).astype(jnp.bfloat16)
    cot_tokens = merge_tokens(cotangent)
    d_coarse = jnp.dot(cot_tokens, w_expand.T, preferred_element_type=jnp.float32).astype(jnp.bfloat16)
    d_hidden = jnp.dot(d_coarse, w_out.T, preferred_element_type=jnp.float32)
    unused, pullback = jax.vjp(activate, act)
    d_act = pullback(d_hidden)[0].astype(jnp.bfloat16)
    grad_out = jnp.dot(hidden.T, d_coarse, preferred_element_type=jnp.float32)
    grad_in = jnp.dot(coarse_normed.T, d_act, preferred_element_type=jnp.float32)
    return (fields_out, grad_in, grad_out)
```

```python
import math

import jax
import jax.numpy as jnp
import numpy as np
from jax import lax
from jax.experimental import pallas as pl
from jax.experimental.pallas import tpu as pltpu
from jax.sharding import PartitionSpec as P

WIN_LON = 6
SHIFT_LON = 3
EPSILON = 1e-05

LEVELS, ROWS, COLS, C1 = 2, 12, 24, 512
TOKENS = LEVELS * ROWS * COLS
HALF = TOKENS // 2
COARSE = TOKENS // 4
EDGE = 48
C2 = 1024
FB = 256
F32 = jnp.float32
BF16 = jnp.bfloat16


def token_tables():
    natural_to_merge = np.zeros(TOKENS, np.int32)
    half_to_edge = np.full(HALF, -1, np.int32)
    edge_to_half = {}
    source_to_window = np.full(2 * HALF + 2 * EDGE, -1, np.int32)
    for level in range(LEVELS):
        for row in range(ROWS):
            for col in range(COLS):
                q = (col % 2) * 2 + row % 2
                h, i3, j = row // 6, row % 6 // 2, col // 2
                merge = q * COARSE + h * 72 + level * 36 + i3 * 12 + j
                natural_to_merge[(level * ROWS + row) * COLS + col] = merge
                if h == 0:
                    place = q * 72 + level * 36 + i3 * 12 + j
                    if col < SHIFT_LON:
                        half_to_edge[place] = level * 18 + row * 3 + col
                        edge_to_half[level * 18 + row * 3 + col] = merge
    for level in range(LEVELS):
        for r in range(ROWS):
            for c in range(COLS):
                window = (c // WIN_LON) * 144 + level * 72 + r * 6 + c % WIN_LON
                row, col = r % 6, c + SHIFT_LON
                if col < COLS:
                    q = (col % 2) * 2 + row % 2
                    place = q * 72 + level * 36 + row // 2 * 12 + col // 2
                    source = place + (HALF if r >= 6 else 0)
                else:
                    source = 2 * HALF + level * 18 + row * 3 + col - COLS
                    source += EDGE if r >= 6 else 0
                source_to_window[source] = window
    window_to_source = np.zeros(TOKENS, np.int32)
    for source, window in enumerate(source_to_window):
        if window >= 0:
            window_to_source[window] = source
    merge_to_natural = np.zeros(TOKENS, np.int32)
    merge_to_natural[natural_to_merge] = np.arange(TOKENS, dtype=np.int32)
    edges_to_merge = np.full(2 * EDGE, -1, np.int32)
    for edge, merge in edge_to_half.items():
        edges_to_merge[edge] = merge + 72
        edges_to_merge[EDGE + edge] = merge
    return natural_to_merge, merge_to_natural, half_to_edge, source_to_window, window_to_source, edges_to_merge


N2M, M2N, H2E, S2W, W2S, E2M = token_tables()


def lanes(table):
    return jnp.asarray(table.reshape(1, -1))


def picks(rows, table):
    spots = lax.broadcasted_iota(jnp.int32, (rows, table.shape[1]), 0)
    return (spots == table).astype(F32).astype(BF16)


def mm(a, b):
    return jnp.dot(a, b, preferred_element_type=F32)


def mm_nt(a, b):
    return lax.dot_general(a, b, (((1,), (1,)), ((), ())), preferred_element_type=F32)


def mm_tn(a, b):
    return lax.dot_general(a, b, (((0,), (0,)), ((), ())), preferred_element_type=F32)


def normed_rows(values, gain):
    center = values - jnp.mean(values, axis=-1, keepdims=True)
    spread = jnp.mean(center * center, axis=-1, keepdims=True)
    return center * lax.rsqrt(spread + EPSILON) * gain


def front_kernel(
    fin, levels, surface, level_table, surface_table, gain, n2m, h2e,
    fields_out, up_out, lo_out, lon_out, diag_out, table,
):
    table[...] = jnp.zeros_like(table)
    table[0:13, :] = level_table[...].astype(F32)
    table[13:15, :] = surface_table[...].astype(F32)
    order = picks(TOKENS, n2m[...])
    spots = lax.broadcasted_iota(jnp.int32, (16, TOKENS), 0)
    hot = ((spots == levels[...]) | (spots == surface[...])).astype(F32).astype(BF16)
    fields = mm(order, fin[...]) + mm(mm_nt(order, hot).astype(BF16), table[...].astype(BF16))
    fields_out[...] = fields
    normed = normed_rows(fields, gain[...].astype(F32))
    up = jnp.concatenate([normed[q * COARSE : q * COARSE + 72] for q in range(4)], axis=0).astype(BF16)
    lo = jnp.concatenate([normed[q * COARSE + 72 : (q + 1) * COARSE] for q in range(4)], axis=0).astype(BF16)
    up_out[...] = up
    lo_out[...] = lo
    edge = picks(EDGE, h2e[...])
    lon_out[...] = mm(edge, lo).astype(BF16)
    diag_out[...] = mm(edge, up).astype(BF16)


def attention_kernel(flag, lo, up, lon, diag, w_qkv, s2w, w2s, lo_out, up_out, lon_out, diag_out, src, qkv, att):
    src[0:HALF, :] = lo[...]
    src[HALF : 2 * HALF, :] = up[...]
    src[2 * HALF : 2 * HALF + EDGE, :] = lon[...]
    src[2 * HALF + EDGE :, :] = diag[...]
    windows = mm(picks(TOKENS, s2w[...]), src[...]).astype(BF16)
    qkv[...] = mm(windows, w_qkv[...]).astype(BF16)
    size = 144
    top = lax.broadcasted_iota(jnp.int32, (size, size), 0)
    left = lax.broadcasted_iota(jnp.int32, (size, size), 1)

    def low(t):
        return ((t >= 36) & (t < 72)) | (t >= 108)

    apart = (low(top) != low(left)) & (flag[0] == 1)
    lane = lax.broadcasted_iota(jnp.int32, (size, 128), 1)
    first = lane < 64
    ones = [jnp.where(first, 1.0, 0.0).astype(BF16), jnp.where(first, 0.0, 1.0).astype(BF16)]
    for w in range(4):
        for pair in range(4):
            rows = slice(w * size, (w + 1) * size)
            cols = pair * 128
            queries = qkv[rows, cols : cols + 128]
            keys = qkv[rows, C1 + cols : C1 + cols + 128]
            values = qkv[rows, 2 * C1 + cols : 2 * C1 + cols + 128]
            total = None
            for side in range(2):
                scores = mm_nt(queries * ones[side], keys) * (1.0 / math.sqrt(64))
                scores = jnp.where(apart, -1e30, scores)
                peak = jnp.max(scores, axis=-1, keepdims=True)
                probs = jnp.exp(scores - peak).astype(BF16)
                both = mm(probs, jnp.concatenate([values * ones[side], ones[side]], axis=1))
                total = both if total is None else total + both
            att[rows, cols : cols + 128] = (total[:, :128] / total[:, 128:]).astype(BF16)
    back = mm(picks(2 * HALF + 2 * EDGE, w2s[...]), att[...]).astype(BF16)
    lo_out[...] = back[0:HALF]
    up_out[...] = back[HALF : 2 * HALF]
    lon_out[...] = back[2 * HALF : 2 * HALF + EDGE]
    diag_out[...] = back[2 * HALF + EDGE :]


def merge_kernel(
    lo, up, lon, diag, fields, w_proj, merge_gain, w_merge, coarse_gain, e2m, skip_out, coarse_out, cn_out
):
    upper, lower = up[...].astype(F32), lo[...].astype(F32)
    parts = []
    for q in range(4):
        parts.append(upper[q * 72 : (q + 1) * 72])
        parts.append(lower[q * 72 : (q + 1) * 72])
    edges = jnp.concatenate([lon[...], diag[...]], axis=0)
    attended = (jnp.concatenate(parts, axis=0) + mm(picks(TOKENS, e2m[...]), edges)).astype(BF16)
    skip = (fields[...] + mm(attended, w_proj[...])).astype(BF16)
    skip_out[...] = skip
    skip = skip.astype(F32)
    blocks = [skip[q * COARSE : (q + 1) * COARSE] for q in range(4)]
    mean = sum(jnp.sum(b, axis=-1, keepdims=True) for b in blocks) * (1.0 / (4 * C1))
    blocks = [b - mean for b in blocks]
    spread = sum(jnp.sum(b * b, axis=-1, keepdims=True) for b in blocks) * (1.0 / (4 * C1))
    scale = lax.rsqrt(spread + EPSILON)
    coarse = None
    for q in range(4):
        gain = merge_gain[0:1, q * C1 : (q + 1) * C1].astype(F32)
        part = mm((blocks[q] * scale * gain).astype(BF16), w_merge[q * C1 : (q + 1) * C1, :])
        coarse = part if coarse is None else coarse + part
    coarse = coarse.astype(BF16)
    coarse_out[...] = coarse
    cn_out[...] = normed_rows(coarse.astype(F32), coarse_gain[...].astype(F32)).astype(BF16)


def cotangent_kernel(cot, w_expand, n2m, dc_out):
    ordered = mm(picks(TOKENS, n2m[...]), cot[...]).astype(BF16)
    total = None
    for q in range(4):
        part = mm_nt(ordered[q * COARSE : (q + 1) * COARSE], w_expand[:, q * C1 : (q + 1) * C1])
        total = part if total is None else total + part
    dc_out[...] = total.astype(BF16)


NEAR = 80
QUAD = 4 * COARSE


def stack_into(full, refs):
    at = 0
    for ref in refs:
        full[at : at + ref.shape[0], :] = ref[...]
        at += ref.shape[0]


def hidden_rows(full, w_in, w_in_far, w_out, w_out_far, hidden_out, slope_out):
    root = math.sqrt(2.0 / math.pi)
    total = None
    for side, (win, wout) in enumerate(((w_in, w_out), (w_in_far, w_out_far))):
        x = mm(full[...], win[...])
        t = jnp.tanh(root * (x + 0.044715 * (x * x * x)))
        half = 0.5 * (1.0 + t)
        hidden = (x * half).astype(BF16)
        slope = half + 0.5 * x * (1.0 - t * t) * (root * (1.0 + 3 * 0.044715 * (x * x)))
        cols = slice(side * FB, (side + 1) * FB)
        hidden_out[:, cols] = hidden
        slope_out[:, cols] = slope.astype(BF16)
        part = mm(hidden, wout[...])
        total = part if total is None else total + part
    return total.astype(BF16)


def near_kernel(own, far, right, left, w_in, w_in_far, w_out, w_out_far, partial, full, hidden, slope):
    stack_into(full, (own, far, right, left))
    partial[...] = hidden_rows(full, w_in, w_in_far, w_out, w_out_far, hidden, slope)


def wide_kernel(
    right, left, far_right2, far_left2, w_in, w_in_far, w_out, w_out_far,
    near_right, near_left, send_right, send_left, full, hidden, slope,
):
    full[0:NEAR, :] = right[0:NEAR, :]
    full[NEAR:COARSE, :] = left[0 : COARSE - NEAR, :]
    full[COARSE : 2 * COARSE, :] = right[NEAR:, :]
    full[2 * COARSE : 3 * COARSE, :] = left[COARSE - NEAR :, :]
    full[3 * COARSE : 3 * COARSE + NEAR, :] = far_right2[...]
    full[3 * COARSE + NEAR :, :] = far_left2[...]
    partial = hidden_rows(full, w_in, w_in_far, w_out, w_out_far, hidden, slope)
    near_right[...] = partial[2 * COARSE : 3 * COARSE]
    near_left[...] = partial[COARSE : 2 * COARSE]
    send_right[0:NEAR, :] = partial[0:NEAR]
    send_right[NEAR:, :] = partial[3 * COARSE : 3 * COARSE + NEAR]
    send_left[0 : COARSE - NEAR, :] = partial[NEAR:COARSE]
    send_left[COARSE - NEAR :, :] = partial[3 * COARSE + NEAR :]


def added(x, y):
    return (x.astype(F32) + y.astype(F32)).astype(BF16)


def pass_kernel(near, far_right, far_left, got_right, got_left, own_r, own_l, far_r, far_l):
    rest = COARSE - NEAR
    own_r[0:NEAR, :] = added(near[3 * COARSE : 3 * COARSE + NEAR, :], got_right[0:NEAR, :])
    own_r[NEAR:, :] = near[3 * COARSE + NEAR :, :]
    own_l[0:NEAR, :] = near[2 * COARSE : 2 * COARSE + NEAR, :]
    own_l[NEAR:, :] = added(near[2 * COARSE + NEAR : 3 * COARSE, :], got_left[0:rest, :])
    far_r[0:NEAR, :] = added(far_right[0:NEAR, :], got_right[NEAR:, :])
    far_r[NEAR:, :] = far_right[NEAR:, :]
    far_l[0:NEAR, :] = far_left[0:NEAR, :]
    far_l[NEAR:, :] = added(far_left[NEAR:, :], got_left[rest:, :])


def far_kernel(near, got_right, got_left, send):
    total = near[COARSE : 2 * COARSE, :].astype(F32) + got_right[...].astype(F32)
    send[...] = (total + got_left[...].astype(F32)).astype(BF16)


def gradient_kernel(
    own, far, right, left, right2, left2, far_right2, far_left2, near_full, near_hidden, near_slope,
    wide_full, wide_hidden, wide_slope, w_out, w_out_far, in_own, in_far, out_own, out_far, dfull, dact,
):
    stack_into(dfull, (own, far, right, left))
    dfull[QUAD : QUAD + NEAR, :] = right2[0:NEAR, :]
    dfull[QUAD + NEAR : QUAD + COARSE, :] = left2[0 : COARSE - NEAR, :]
    dfull[QUAD + COARSE : QUAD + 2 * COARSE, :] = right2[NEAR:, :]
    dfull[QUAD + 2 * COARSE : QUAD + 3 * COARSE, :] = left2[COARSE - NEAR :, :]
    dfull[QUAD + 3 * COARSE : QUAD + 3 * COARSE + NEAR, :] = far_right2[...]
    dfull[QUAD + 3 * COARSE + NEAR :, :] = far_left2[...]
    for side, wout in enumerate((w_out, w_out_far)):
        cols = slice(side * FB, (side + 1) * FB)
        for part, slope in enumerate((near_slope, wide_slope)):
            rows = slice(part * QUAD, (part + 1) * QUAD)
            back = mm_nt(dfull[rows, :], wout[...])
            dact[rows, cols] = (back * slope[:, cols].astype(F32)).astype(BF16)
    for at in range(0, C2, 256):
        c = slice(at, at + 256)
        both = mm_tn(dfull[0:QUAD, c], near_hidden[...]) + mm_tn(dfull[QUAD:, c], wide_hidden[...])
        out_own[c, :] = both[:, :FB].astype(BF16)
        out_far[c, :] = both[:, FB:].astype(BF16)
        both = mm_tn(near_full[:, c], dact[0:QUAD, :]) + mm_tn(wide_full[:, c], dact[QUAD:, :])
        in_own[c, :] = both[:, :FB].astype(BF16)
        in_far[c, :] = both[:, FB:].astype(BF16)


def expand_kernel(coarse, near, got_right, got_left, got_far, w_expand, skip, m2n, fields_out):
    mixed = near[0:COARSE, :].astype(F32) + got_right[...].astype(F32)
    mixed = mixed + (got_left[...].astype(F32) + got_far[...].astype(F32))
    coarse_out = (coarse[...].astype(F32) + mixed).astype(BF16)
    parts = []
    for q in range(4):
        expanded = mm(coarse_out, w_expand[:, q * C1 : (q + 1) * C1])
        parts.append((skip[q * COARSE : (q + 1) * COARSE, :].astype(F32) + expanded).astype(BF16))
    fields_out[...] = mm(picks(TOKENS, m2n[...]), jnp.concatenate(parts, axis=0)).astype(BF16)


def shaped(dims, dtype=BF16):
    return jax.ShapeDtypeStruct(dims, dtype)


def run(kernel, outs, args, flops, scratch=(), smem=()):
    nbytes = sum(a.size * a.dtype.itemsize for a in args) + sum(math.prod(o.shape) * 2 for o in outs)
    return pl.pallas_call(
        kernel,
        out_shape=tuple(outs),
        in_specs=[pl.BlockSpec(memory_space=pltpu.SMEM if k in smem else pltpu.VMEM) for k in range(len(args))],
        out_specs=tuple(pl.BlockSpec(memory_space=pltpu.VMEM) for _ in outs),
        scratch_shapes=list(scratch),
        cost_estimate=pl.CostEstimate(flops=int(flops), bytes_accessed=int(nbytes), transcendentals=0),
    )(*args)


def lat_of(y, x, core):
    return (y % 2) * 8 + (x % 4) * 2 + core % 2


def lat_moves(dy, dx, dcore):
    return [(l, lat_of(l // 8 + dy, l // 2 % 4 + dx, l % 2 + dcore)) for l in range(16)]


def on_lat(value, dy=0, dx=0, dcore=0):
    return lax.ppermute(value, "lat", lat_moves(dy, dx, dcore))


def shift(value, axes, steps):
    if axes == "both":
        pairs = [
            (o * 16 + l, (o + steps) % 16 * 16 + (l + steps) % 16) for o in range(16) for l in range(16)
        ]
        return lax.ppermute(value, ("lon", "lat"), pairs)
    return lax.ppermute(value, axes, [(s, (s + steps) % 16) for s in range(16)])


def gathered(block):
    far = on_lat(block, dy=1)
    right, left = on_lat(block, dx=1), on_lat(block, dx=-1)
    right2 = on_lat(jnp.concatenate([right[:NEAR], far], axis=0), dx=1)
    left2 = on_lat(jnp.concatenate([left[NEAR:], far], axis=0), dx=-1)
    far_right2, far_left2 = on_lat(right2[NEAR : 2 * NEAR], dx=1), on_lat(left2[COARSE:], dx=-1)
    return (block, far, right, left), (right2, left2, far_right2, far_left2)


EIGHTS = [[half * 8 + z for z in range(8)] for half in range(2)]


def whole(
    fields_in, level_map, land_sea, level_table, surface_table, norm_gain, w_qkv, w_proj, merge_gain,
    w_merge, coarse_gain, w_in, w_out, w_expand, cotangent,
):
    lat, lon_index = lax.axis_index("lat"), lax.axis_index("lon")
    surface = 13 + (land_sea.reshape(1, HALF) == 1).astype(jnp.int32)
    w_in_far, w_out_far = on_lat(w_in, dcore=1), on_lat(w_out, dcore=1)
    fields, up, lo, lon, diag = run(
        front_kernel,
        [shaped((TOKENS, C1), F32), shaped((HALF, C1)), shaped((HALF, C1)), shaped((EDGE, C1)), shaped((EDGE, C1))],
        (
            fields_in.reshape(TOKENS, C1), level_map.reshape(1, TOKENS), jnp.concatenate([surface, surface], axis=1),
            level_table, surface_table, norm_gain.reshape(1, C1), lanes(N2M), lanes(H2E),
        ),
        4e8,
        [pltpu.VMEM((16, C1), F32)],
    )
    up, lon, diag = shift(up, "lat", -1), shift(lon, "lon", -1), shift(diag, "both", -1)
    (dc,) = run(cotangent_kernel, [shaped((COARSE, C2))], (cotangent.reshape(TOKENS, C1), w_expand, lanes(N2M)), 1e9)
    dc_near, dc_wide = gathered(dc)
    flag = (lat == 15).astype(jnp.int32).reshape(1)
    lo, up, lon, diag = run(
        attention_kernel,
        [shaped((HALF, C1)), shaped((HALF, C1)), shaped((EDGE, C1)), shaped((EDGE, C1))],
        (flag, lo, up, lon, diag, w_qkv, lanes(S2W), lanes(W2S)),
        3e9,
        [pltpu.VMEM((2 * HALF + 2 * EDGE, C1), BF16), pltpu.VMEM((TOKENS, 3 * C1), BF16), pltpu.VMEM((TOKENS, C1), BF16)],
        smem=(0,),
    )
    up, lon, diag = shift(up, "lat", 1), shift(lon, "lon", 1), shift(diag, "both", 1)
    skip, coarse, cn = run(
        merge_kernel,
        [shaped((TOKENS, C1)), shaped((COARSE, C2)), shaped((COARSE, C2))],
        (lo, up, lon, diag, fields, w_proj, merge_gain.reshape(1, 4 * C1), w_merge, coarse_gain.reshape(1, C2), lanes(E2M)),
        2e9,
    )
    cn_near, cn_wide = gathered(cn)
    weights = (w_in, w_in_far, w_out, w_out_far)
    kept = [shaped((QUAD, C2)), shaped((QUAD, 2 * FB)), shaped((QUAD, 2 * FB))]
    near, *near_kept = run(near_kernel, [shaped((QUAD, C2)), *kept], (*cn_near, *weights), 2.5e9)
    far_right, far_left, to_right, to_left, *wide_kept = run(
        wide_kernel,
        [shaped((COARSE, C2)), shaped((COARSE, C2)), shaped((2 * NEAR, C2)), shaped((2 * (COARSE - NEAR), C2)), *kept],
        (*cn_wide, *weights),
        2.5e9,
    )
    got_right, got_left = on_lat(to_right, dx=1), on_lat(to_left, dx=-1)
    in_own, in_far, out_own, out_far = run(
        gradient_kernel,
        [shaped((C2, FB))] * 4,
        (*dc_near, *dc_wide, *near_kept, *wide_kept, w_out, w_out_far),
        4e9,
        [pltpu.VMEM((8 * COARSE, C2), BF16), pltpu.VMEM((8 * COARSE, 2 * FB), BF16)],
    )
    own_r, own_l, far_r, far_l = run(
        pass_kernel, [shaped((COARSE, C2))] * 4, (near, far_right, far_left, got_right, got_left), 1e8
    )
    far_r, far_l = on_lat(far_r, dx=1), on_lat(far_l, dx=-1)
    own_r, own_l = on_lat(own_r, dx=1), on_lat(own_l, dx=-1)
    (across,) = run(far_kernel, [shaped((COARSE, C2))], (near, far_r, far_l), 1e8)
    across = on_lat(across, dy=1)

    out_sum, in_sum = added(out_own, on_lat(out_far, dcore=1)), added(in_own, on_lat(in_far, dcore=1))
    both = jnp.stack([out_sum.reshape(2, 8, 64, FB), in_sum.reshape(2, 8, 64, FB)], axis=2)
    side = lon_index // 8
    mine = lax.dynamic_index_in_dim(both, side, 0, keepdims=False)
    other = lax.dynamic_index_in_dim(both, 1 - side, 0, keepdims=False)
    other = lax.ppermute(other, "lon", [(o, (o + 8) % 16) for o in range(16)])
    pieces = lax.all_to_all(added(mine, other), "lon", 0, 0, axis_index_groups=EIGHTS, tiled=True)
    total = jnp.sum(pieces.astype(F32), axis=0)
    grad_out, grad_in = total[0].T, total[1]
    (fields_out,) = run(
        expand_kernel,
        [shaped((TOKENS, C1))],
        (coarse, near, own_r, own_l, across, w_expand, skip, lanes(M2N)),
        1e9,
    )
    return (fields_out.reshape(LEVELS, ROWS, COLS, C1), grad_in, grad_out)


def solution(mesh):
    placed = (
        P(None, "lat", "lon", None),
        P(None, "lat", "lon"),
        P("lat", "lon"),
        P(),
        P(),
        P(),
        P(),
        P(),
        P(),
        P(),
        P(),
        P(None, "lat"),
        P("lat", None),
        P(),
        P(None, "lat", "lon", None),
    )
    return jax.shard_map(
        whole,
        mesh=mesh,
        in_specs=placed,
        out_specs=(P(None, "lat", "lon", None), P("lon", "lat"), P("lat", "lon")),
        check_vma=False,
    )
```

```python
import math

import jax
import jax.numpy as jnp
import numpy as np
from jax import lax
from jax.experimental import pallas as pl
from jax.experimental.pallas import tpu as pltpu
from jax.sharding import PartitionSpec as P


WIN_LON = 6
SHIFT_LON = 3
EPSILON = 1e-05

LEVELS, ROWS, COLS, C1 = 2, 12, 24, 512
TOKENS = LEVELS * ROWS * COLS
HALF = TOKENS // 2
COARSE = TOKENS // 4
EDGE = 48
C2 = 1024
FB = 256
F32 = jnp.float32
BF16 = jnp.bfloat16


def token_tables():
    natural_to_merge = np.zeros(TOKENS, np.int32)
    half_to_edge = np.full(HALF, -1, np.int32)
    edge_to_half = {}
    source_to_window = np.full(2 * HALF + 2 * EDGE, -1, np.int32)
    for level in range(LEVELS):
        for row in range(ROWS):
            for col in range(COLS):
                q = (col % 2) * 2 + row % 2
                h, i3, j = row // 6, row % 6 // 2, col // 2
                merge = q * COARSE + h * 72 + level * 36 + i3 * 12 + j
                natural_to_merge[(level * ROWS + row) * COLS + col] = merge
                if h == 0:
                    place = q * 72 + level * 36 + i3 * 12 + j
                    if col < SHIFT_LON:
                        half_to_edge[place] = level * 18 + row * 3 + col
                        edge_to_half[level * 18 + row * 3 + col] = merge
    for level in range(LEVELS):
        for r in range(ROWS):
            for c in range(COLS):
                window = (c // WIN_LON) * 144 + level * 72 + r * 6 + c % WIN_LON
                row, col = r % 6, c + SHIFT_LON
                if col < COLS:
                    q = (col % 2) * 2 + row % 2
                    place = q * 72 + level * 36 + row // 2 * 12 + col // 2
                    source = place + (HALF if r >= 6 else 0)
                else:
                    source = 2 * HALF + level * 18 + row * 3 + col - COLS
                    source += EDGE if r >= 6 else 0
                source_to_window[source] = window
    window_to_source = np.zeros(TOKENS, np.int32)
    for source, window in enumerate(source_to_window):
        if window >= 0:
            window_to_source[window] = source
    merge_to_natural = np.zeros(TOKENS, np.int32)
    merge_to_natural[natural_to_merge] = np.arange(TOKENS, dtype=np.int32)
    edges_to_merge = np.full(2 * EDGE, -1, np.int32)
    for edge, merge in edge_to_half.items():
        edges_to_merge[edge] = merge + 72
        edges_to_merge[EDGE + edge] = merge
    return natural_to_merge, merge_to_natural, half_to_edge, source_to_window, window_to_source, edges_to_merge


N2M, M2N, H2E, S2W, W2S, E2M = token_tables()


def lanes(table):
    return jnp.asarray(table.reshape(1, -1))


def picks(rows, table):
    spots = lax.broadcasted_iota(jnp.int32, (rows, table.shape[1]), 0)
    return (spots == table).astype(F32).astype(BF16)


def mm(a, b):
    return jnp.dot(a, b, preferred_element_type=F32)


def mm_nt(a, b):
    return lax.dot_general(a, b, (((1,), (1,)), ((), ())), preferred_element_type=F32)


def mm_tn(a, b):
    return lax.dot_general(a, b, (((0,), (0,)), ((), ())), preferred_element_type=F32)


def normed_rows(values, gain):
    center = values - jnp.mean(values, axis=-1, keepdims=True)
    spread = jnp.mean(center * center, axis=-1, keepdims=True)
    return center * lax.rsqrt(spread + EPSILON) * gain


def front_kernel(
    fin, ids, level_table, surface_table, gain, n2m, h2e,
    fields_out, up_out, lo_out, lon_out, diag_out, table,
):
    table[...] = jnp.zeros_like(table)
    table[0:13, :] = level_table[...].astype(F32)
    table[13:15, :] = surface_table[...].astype(F32)
    order = picks(TOKENS, n2m[...])
    spots = lax.broadcasted_iota(jnp.int32, (16, TOKENS), 0)
    hot = ((spots == ids[0:1, :]) | (spots == ids[1:2, :])).astype(F32).astype(BF16)
    fields = mm(order, fin[...]) + mm(mm_nt(order, hot).astype(BF16), table[...].astype(BF16))
    fields_out[...] = fields
    normed = normed_rows(fields, gain[...].astype(F32))
    up = jnp.concatenate([normed[q * COARSE : q * COARSE + 72] for q in range(4)], axis=0).astype(BF16)
    lo = jnp.concatenate([normed[q * COARSE + 72 : (q + 1) * COARSE] for q in range(4)], axis=0).astype(BF16)
    up_out[...] = up
    lo_out[...] = lo
    edge = picks(EDGE, h2e[...])
    lon_out[...] = mm(edge, lo).astype(BF16)
    diag_out[...] = mm(edge, up).astype(BF16)


def attention_kernel(flag, lo, up, lon, diag, w_qkv, s2w, w2s, lo_out, up_out, lon_out, diag_out, src, qkv, att):
    src[0:HALF, :] = lo[...]
    src[HALF : 2 * HALF, :] = up[...]
    src[2 * HALF : 2 * HALF + EDGE, :] = lon[...]
    src[2 * HALF + EDGE :, :] = diag[...]
    windows = mm(picks(TOKENS, s2w[...]), src[...]).astype(BF16)
    qkv[...] = mm(windows, w_qkv[...]).astype(BF16)
    size = 144
    top = lax.broadcasted_iota(jnp.int32, (size, size), 0)
    left = lax.broadcasted_iota(jnp.int32, (size, size), 1)

    def low(t):
        return ((t >= 36) & (t < 72)) | (t >= 108)

    apart = (low(top) != low(left)) & (flag[0] == 1)
    lane = lax.broadcasted_iota(jnp.int32, (size, 128), 1)
    first = lane < 64
    ones = [jnp.where(first, 1.0, 0.0).astype(BF16), jnp.where(first, 0.0, 1.0).astype(BF16)]

    def one_window(w, carry):
        rows = pl.ds(pl.multiple_of(w * size, 16), size)
        for pair in range(4):
            cols = pair * 128
            queries = qkv[rows, cols : cols + 128]
            keys = qkv[rows, C1 + cols : C1 + cols + 128]
            values = qkv[rows, 2 * C1 + cols : 2 * C1 + cols + 128]
            total = None
            for side in range(2):
                scores = mm_nt(queries * ones[side], keys) * (1.0 / math.sqrt(64))
                scores = jnp.where(apart, -1e30, scores)
                peak = jnp.max(scores, axis=-1, keepdims=True)
                probs = jnp.exp(scores - peak).astype(BF16)
                both = mm(probs, jnp.concatenate([values * ones[side], ones[side]], axis=1))
                total = both if total is None else total + both
            att[rows, cols : cols + 128] = (total[:, :128] / total[:, 128:]).astype(BF16)
        return carry

    lax.fori_loop(0, 4, one_window, 0)
    back = mm(picks(2 * HALF + 2 * EDGE, w2s[...]), att[...]).astype(BF16)
    lo_out[...] = back[0:HALF]
    up_out[...] = back[HALF : 2 * HALF]
    lon_out[...] = back[2 * HALF : 2 * HALF + EDGE]
    diag_out[...] = back[2 * HALF + EDGE :]


def merge_kernel(
    lo, up, lon, diag, fields, w_proj, merge_gain, w_merge, coarse_gain, e2m, skip_out, coarse_out, cn_out
):
    upper, lower = up[...].astype(F32), lo[...].astype(F32)
    parts = []
    for q in range(4):
        parts.append(upper[q * 72 : (q + 1) * 72])
        parts.append(lower[q * 72 : (q + 1) * 72])
    edges = jnp.concatenate([lon[...], diag[...]], axis=0)
    attended = (jnp.concatenate(parts, axis=0) + mm(picks(TOKENS, e2m[...]), edges)).astype(BF16)
    skip = (fields[...] + mm(attended, w_proj[...])).astype(BF16)
    skip_out[...] = skip
    skip = skip.astype(F32)
    blocks = [skip[q * COARSE : (q + 1) * COARSE] for q in range(4)]
    mean = sum(jnp.sum(b, axis=-1, keepdims=True) for b in blocks) * (1.0 / (4 * C1))
    blocks = [b - mean for b in blocks]
    spread = sum(jnp.sum(b * b, axis=-1, keepdims=True) for b in blocks) * (1.0 / (4 * C1))
    scale = lax.rsqrt(spread + EPSILON)
    coarse = None
    for q in range(4):
        gain = merge_gain[0:1, q * C1 : (q + 1) * C1].astype(F32)
        part = mm((blocks[q] * scale * gain).astype(BF16), w_merge[q * C1 : (q + 1) * C1, :])
        coarse = part if coarse is None else coarse + part
    coarse = coarse.astype(BF16)
    coarse_out[...] = coarse
    cn_out[...] = normed_rows(coarse.astype(F32), coarse_gain[...].astype(F32)).astype(BF16)


def cotangent_kernel(cot, w_expand, n2m, dc_out, ordered, total):
    ordered[...] = mm(picks(TOKENS, n2m[...]), cot[...]).astype(BF16)
    total[...] = jnp.zeros_like(total)

    def one_place(q, carry):
        rows = pl.ds(pl.multiple_of(q * COARSE, 16), COARSE)
        cols = pl.ds(pl.multiple_of(q * C1, C1), C1)
        total[...] += mm_nt(ordered[rows, :], w_expand[:, cols])
        return carry

    lax.fori_loop(0, 4, one_place, 0)
    dc_out[...] = total[...].astype(BF16)


NEAR = 80
QUAD = 4 * COARSE


def stack_into(full, refs):
    at = 0
    for ref in refs:
        full[at : at + ref.shape[0], :] = ref[...]
        at += ref.shape[0]


def hidden_rows(full, w_in, w_in_far, w_out, w_out_far, hidden_out, slope_out, partial):
    root = math.sqrt(2.0 / math.pi)

    def one_part(k, carry):
        rows = pl.ds(pl.multiple_of(k * (QUAD // 2), 32), QUAD // 2)
        total = None
        for side, (win, wout) in enumerate(((w_in, w_out), (w_in_far, w_out_far))):
            x = mm(full[rows, :], win[...])
            t = jnp.tanh(root * (x + 0.044715 * (x * x * x)))
            half = 0.5 * (1.0 + t)
            hidden = (x * half).astype(BF16)
            slope = half + 0.5 * x * (1.0 - t * t) * (root * (1.0 + 3 * 0.044715 * (x * x)))
            cols = slice(side * FB, (side + 1) * FB)
            hidden_out[rows, cols] = hidden
            slope_out[rows, cols] = slope.astype(BF16)
            part = mm(hidden, wout[...])
            total = part if total is None else total + part
        partial[rows, :] = total.astype(BF16)
        return carry

    lax.fori_loop(0, 2, one_part, 0)


def near_kernel(own, far, right, left, w_in, w_in_far, w_out, w_out_far, partial, full, hidden, slope):
    stack_into(full, (own, far, right, left))
    hidden_rows(full, w_in, w_in_far, w_out, w_out_far, hidden, slope, partial)


def wide_kernel(
    right, left, far_right2, far_left2, w_in, w_in_far, w_out, w_out_far,
    near_right, near_left, send_right, send_left, full, hidden, slope, partial,
):
    full[0:NEAR, :] = right[0:NEAR, :]
    full[NEAR:COARSE, :] = left[0 : COARSE - NEAR, :]
    full[COARSE : 2 * COARSE, :] = right[NEAR:, :]
    full[2 * COARSE : 3 * COARSE, :] = left[COARSE - NEAR :, :]
    full[3 * COARSE : 3 * COARSE + NEAR, :] = far_right2[...]
    full[3 * COARSE + NEAR :, :] = far_left2[...]
    hidden_rows(full, w_in, w_in_far, w_out, w_out_far, hidden, slope, partial)
    near_right[...] = partial[2 * COARSE : 3 * COARSE, :]
    near_left[...] = partial[COARSE : 2 * COARSE, :]
    send_right[0:NEAR, :] = partial[0:NEAR, :]
    send_right[NEAR:, :] = partial[3 * COARSE : 3 * COARSE + NEAR, :]
    send_left[0 : COARSE - NEAR, :] = partial[NEAR:COARSE, :]
    send_left[COARSE - NEAR :, :] = partial[3 * COARSE + NEAR :, :]


def added(x, y):
    return (x.astype(F32) + y.astype(F32)).astype(BF16)


def pass_kernel(near, far_right, far_left, got_right, got_left, own_r, own_l, far_r, far_l):
    rest = COARSE - NEAR
    own_r[0:NEAR, :] = added(near[3 * COARSE : 3 * COARSE + NEAR, :], got_right[0:NEAR, :])
    own_r[NEAR:, :] = near[3 * COARSE + NEAR :, :]
    own_l[0:NEAR, :] = near[2 * COARSE : 2 * COARSE + NEAR, :]
    own_l[NEAR:, :] = added(near[2 * COARSE + NEAR : 3 * COARSE, :], got_left[0:rest, :])
    far_r[0:NEAR, :] = added(far_right[0:NEAR, :], got_right[NEAR:, :])
    far_r[NEAR:, :] = far_right[NEAR:, :]
    far_l[0:NEAR, :] = far_left[0:NEAR, :]
    far_l[NEAR:, :] = added(far_left[NEAR:, :], got_left[rest:, :])


def far_kernel(near, got_right, got_left, send):
    total = near[COARSE : 2 * COARSE, :].astype(F32) + got_right[...].astype(F32)
    send[...] = (total + got_left[...].astype(F32)).astype(BF16)


def gradient_kernel(
    own, far, right, left, right2, left2, far_right2, far_left2, near_full, near_hidden, near_slope,
    wide_full, wide_hidden, wide_slope, w_out, w_out_far, in_own, in_far, out_own, out_far, dfull, dact,
):
    stack_into(dfull, (own, far, right, left))
    dfull[QUAD : QUAD + NEAR, :] = right2[0:NEAR, :]
    dfull[QUAD + NEAR : QUAD + COARSE, :] = left2[0 : COARSE - NEAR, :]
    dfull[QUAD + COARSE : QUAD + 2 * COARSE, :] = right2[NEAR:, :]
    dfull[QUAD + 2 * COARSE : QUAD + 3 * COARSE, :] = left2[COARSE - NEAR :, :]
    dfull[QUAD + 3 * COARSE : QUAD + 3 * COARSE + NEAR, :] = far_right2[...]
    dfull[QUAD + 3 * COARSE + NEAR :, :] = far_left2[...]
    for side, wout in enumerate((w_out, w_out_far)):
        cols = slice(side * FB, (side + 1) * FB)
        for part, slope in enumerate((near_slope, wide_slope)):
            rows = slice(part * QUAD, (part + 1) * QUAD)
            back = mm_nt(dfull[rows, :], wout[...])
            dact[rows, cols] = (back * slope[:, cols].astype(F32)).astype(BF16)

    def one_block(k, carry):
        c = pl.ds(pl.multiple_of(k * 256, 256), 256)
        both = mm_tn(dfull[0:QUAD, c], near_hidden[...]) + mm_tn(dfull[QUAD:, c], wide_hidden[...])
        out_own[c, :] = both[:, :FB].astype(BF16)
        out_far[c, :] = both[:, FB:].astype(BF16)
        both = mm_tn(near_full[:, c], dact[0:QUAD, :]) + mm_tn(wide_full[:, c], dact[QUAD:, :])
        in_own[c, :] = both[:, :FB].astype(BF16)
        in_far[c, :] = both[:, FB:].astype(BF16)
        return carry

    lax.fori_loop(0, 4, one_block, 0)


def expand_kernel(coarse, near, got_right, got_left, got_far, w_expand, skip, m2n, fields_out, parts):
    mixed = near[0:COARSE, :].astype(F32) + got_right[...].astype(F32)
    mixed = mixed + (got_left[...].astype(F32) + got_far[...].astype(F32))
    coarse_out = (coarse[...].astype(F32) + mixed).astype(BF16)

    def one_place(q, carry):
        rows = pl.ds(pl.multiple_of(q * COARSE, 16), COARSE)
        cols = pl.ds(pl.multiple_of(q * C1, C1), C1)
        parts[rows, :] = (skip[rows, :].astype(F32) + mm(coarse_out, w_expand[:, cols])).astype(BF16)
        return carry

    lax.fori_loop(0, 4, one_place, 0)
    fields_out[...] = mm(picks(TOKENS, m2n[...]), parts[...]).astype(BF16)


def shaped(dims, dtype=BF16):
    return jax.ShapeDtypeStruct(dims, dtype)


def run(kernel, outs, args, flops, scratch=(), smem=()):
    nbytes = sum(a.size * a.dtype.itemsize for a in args) + sum(math.prod(o.shape) * 2 for o in outs)
    return pl.pallas_call(
        kernel,
        out_shape=tuple(outs),
        in_specs=[pl.BlockSpec(memory_space=pltpu.SMEM if k in smem else pltpu.VMEM) for k in range(len(args))],
        out_specs=tuple(pl.BlockSpec(memory_space=pltpu.VMEM) for _ in outs),
        scratch_shapes=list(scratch),
        compiler_params=pltpu.CompilerParams(vmem_limit_bytes=32 * 1024 * 1024),
        cost_estimate=pl.CostEstimate(flops=int(flops), bytes_accessed=int(nbytes), transcendentals=0),
    )(*args)


def lat_of(y, x, core):
    return (y % 2) * 8 + (x % 4) * 2 + core % 2


def lat_moves(dy, dx, dcore):
    return [(l, lat_of(l // 8 + dy, l // 2 % 4 + dx, l % 2 + dcore)) for l in range(16)]


def on_lat(value, dy=0, dx=0, dcore=0):
    return lax.ppermute(value, "lat", lat_moves(dy, dx, dcore))


def shift(value, axes, steps):
    if axes == "both":
        pairs = [
            (o * 16 + l, (o + steps) % 16 * 16 + (l + steps) % 16) for o in range(16) for l in range(16)
        ]
        return lax.ppermute(value, ("lon", "lat"), pairs)
    return lax.ppermute(value, axes, [(s, (s + steps) % 16) for s in range(16)])


def gathered(block):
    far = on_lat(block, dy=1)
    right, left = on_lat(block, dx=1), on_lat(block, dx=-1)
    right2 = on_lat(jnp.concatenate([right[:NEAR], far], axis=0), dx=1)
    left2 = on_lat(jnp.concatenate([left[NEAR:], far], axis=0), dx=-1)
    far_right2, far_left2 = on_lat(right2[NEAR : 2 * NEAR], dx=1), on_lat(left2[COARSE:], dx=-1)
    return (block, far, right, left), (right2, left2, far_right2, far_left2)


EIGHTS = [[half * 8 + z for z in range(8)] for half in range(2)]


def whole(
    fields_in, level_map, land_sea, level_table, surface_table, norm_gain, w_qkv, w_proj, merge_gain,
    w_merge, coarse_gain, w_in, w_out, w_expand, cotangent,
):
    lat, lon_index = lax.axis_index("lat"), lax.axis_index("lon")
    surface = 13 + (land_sea == 1).astype(jnp.int32)
    ids = jnp.concatenate([level_map.reshape(2 * ROWS, COLS), surface, surface], axis=0).reshape(2, TOKENS)
    w_in_far, w_out_far = on_lat(w_in, dcore=1), on_lat(w_out, dcore=1)
    fields, up, lo, lon, diag = run(
        front_kernel,
        [shaped((TOKENS, C1), F32), shaped((HALF, C1)), shaped((HALF, C1)), shaped((EDGE, C1)), shaped((EDGE, C1))],
        (
            fields_in.reshape(TOKENS, C1), ids,
            level_table, surface_table, norm_gain.reshape(1, C1), lanes(N2M), lanes(H2E),
        ),
        4e8,
        [pltpu.VMEM((16, C1), F32)],
    )
    up, lon, diag = shift(up, "lat", -1), shift(lon, "lon", -1), shift(diag, "both", -1)
    (dc,) = run(
        cotangent_kernel, [shaped((COARSE, C2))], (cotangent.reshape(TOKENS, C1), w_expand, lanes(N2M)), 1e9,
        [pltpu.VMEM((TOKENS, C1), BF16), pltpu.VMEM((COARSE, C2), F32)],
    )
    dc_near, dc_wide = gathered(dc)
    flag = (lat == 15).astype(jnp.int32).reshape(1)
    lo, up, lon, diag = run(
        attention_kernel,
        [shaped((HALF, C1)), shaped((HALF, C1)), shaped((EDGE, C1)), shaped((EDGE, C1))],
        (flag, lo, up, lon, diag, w_qkv, lanes(S2W), lanes(W2S)),
        3e9,
        [pltpu.VMEM((2 * HALF + 2 * EDGE, C1), BF16), pltpu.VMEM((TOKENS, 3 * C1), BF16), pltpu.VMEM((TOKENS, C1), BF16)],
        smem=(0,),
    )
    up, lon, diag = shift(up, "lat", 1), shift(lon, "lon", 1), shift(diag, "both", 1)
    skip, coarse, cn = run(
        merge_kernel,
        [shaped((TOKENS, C1)), shaped((COARSE, C2)), shaped((COARSE, C2))],
        (lo, up, lon, diag, fields, w_proj, merge_gain.reshape(1, 4 * C1), w_merge, coarse_gain.reshape(1, C2), lanes(E2M)),
        2e9,
    )
    cn_near, cn_wide = gathered(cn)
    weights = (w_in, w_in_far, w_out, w_out_far)
    kept = [shaped((QUAD, C2)), shaped((QUAD, 2 * FB)), shaped((QUAD, 2 * FB))]
    near, *near_kept = run(near_kernel, [shaped((QUAD, C2)), *kept], (*cn_near, *weights), 2.5e9)
    far_right, far_left, to_right, to_left, *wide_kept = run(
        wide_kernel,
        [shaped((COARSE, C2)), shaped((COARSE, C2)), shaped((2 * NEAR, C2)), shaped((2 * (COARSE - NEAR), C2)), *kept],
        (*cn_wide, *weights),
        2.5e9,
        [pltpu.VMEM((QUAD, C2), BF16)],
    )
    got_right, got_left = on_lat(to_right, dx=1), on_lat(to_left, dx=-1)
    in_own, in_far, out_own, out_far = run(
        gradient_kernel,
        [shaped((C2, FB))] * 4,
        (*dc_near, *dc_wide, *near_kept, *wide_kept, w_out, w_out_far),
        4e9,
        [pltpu.VMEM((8 * COARSE, C2), BF16), pltpu.VMEM((8 * COARSE, 2 * FB), BF16)],
    )
    own_r, own_l, far_r, far_l = run(
        pass_kernel, [shaped((COARSE, C2))] * 4, (near, far_right, far_left, got_right, got_left), 1e8
    )
    far_r, far_l = on_lat(far_r, dx=1), on_lat(far_l, dx=-1)
    own_r, own_l = on_lat(own_r, dx=1), on_lat(own_l, dx=-1)
    (across,) = run(far_kernel, [shaped((COARSE, C2))], (near, far_r, far_l), 1e8)
    across = on_lat(across, dy=1)

    out_sum, in_sum = added(out_own, on_lat(out_far, dcore=1)), added(in_own, on_lat(in_far, dcore=1))
    both = jnp.stack([out_sum.reshape(2, 8, 64, FB), in_sum.reshape(2, 8, 64, FB)], axis=2)
    side = lon_index // 8
    mine = lax.dynamic_index_in_dim(both, side, 0, keepdims=False)
    other = lax.dynamic_index_in_dim(both, 1 - side, 0, keepdims=False)
    other = lax.ppermute(other, "lon", [(o, (o + 8) % 16) for o in range(16)])
    pieces = lax.all_to_all(added(mine, other), "lon", 0, 0, axis_index_groups=EIGHTS, tiled=True)
    total = jnp.sum(pieces.astype(F32), axis=0)
    grad_out, grad_in = total[0].T, total[1]
    (fields_out,) = run(
        expand_kernel,
        [shaped((TOKENS, C1))],
        (coarse, near, own_r, own_l, across, w_expand, skip, lanes(M2N)),
        1e9,
        [pltpu.VMEM((TOKENS, C1), BF16)],
    )
    return (fields_out.reshape(LEVELS, ROWS, COLS, C1), grad_in, grad_out)


def solution(mesh):
    placed = (
        P(None, "lat", "lon", None),
        P(None, "lat", "lon"),
        P("lat", "lon"),
        P(),
        P(),
        P(),
        P(),
        P(),
        P(),
        P(),
        P(),
        P(None, "lat"),
        P("lat", None),
        P(),
        P(None, "lat", "lon", None),
    )
    return jax.shard_map(
        whole,
        mesh=mesh,
        in_specs=placed,
        out_specs=(P(None, "lat", "lon", None), P("lon", "lat"), P("lat", "lon")),
        check_vma=False,
    )
```

```python
import math

import jax
import jax.numpy as jnp
import numpy as np
from jax import lax
from jax.experimental import pallas as pl
from jax.experimental.pallas import tpu as pltpu
from jax.sharding import PartitionSpec as P


WIN_LON = 6
SHIFT_LON = 3
EPSILON = 1e-05

LEVELS, ROWS, COLS, C1 = 2, 12, 24, 512
TOKENS = LEVELS * ROWS * COLS
HALF = TOKENS // 2
COARSE = TOKENS // 4
EDGE = 48
C2 = 1024
FB = 256
F32 = jnp.float32
BF16 = jnp.bfloat16


def token_tables():
    natural_to_merge = np.zeros(TOKENS, np.int32)
    half_to_edge = np.full(HALF, -1, np.int32)
    edge_to_half = {}
    source_to_window = np.full(2 * HALF + 2 * EDGE, -1, np.int32)
    for level in range(LEVELS):
        for row in range(ROWS):
            for col in range(COLS):
                q = (col % 2) * 2 + row % 2
                h, i3, j = row // 6, row % 6 // 2, col // 2
                merge = q * COARSE + h * 72 + level * 36 + i3 * 12 + j
                natural_to_merge[(level * ROWS + row) * COLS + col] = merge
                if h == 0:
                    place = q * 72 + level * 36 + i3 * 12 + j
                    if col < SHIFT_LON:
                        half_to_edge[place] = level * 18 + row * 3 + col
                        edge_to_half[level * 18 + row * 3 + col] = merge
    for level in range(LEVELS):
        for r in range(ROWS):
            for c in range(COLS):
                window = (c // WIN_LON) * 144 + level * 72 + r * 6 + c % WIN_LON
                row, col = r % 6, c + SHIFT_LON
                if col < COLS:
                    q = (col % 2) * 2 + row % 2
                    place = q * 72 + level * 36 + row // 2 * 12 + col // 2
                    source = place + (HALF if r >= 6 else 0)
                else:
                    source = 2 * HALF + level * 18 + row * 3 + col - COLS
                    source += EDGE if r >= 6 else 0
                source_to_window[source] = window
    window_to_source = np.zeros(TOKENS, np.int32)
    for source, window in enumerate(source_to_window):
        if window >= 0:
            window_to_source[window] = source
    merge_to_natural = np.zeros(TOKENS, np.int32)
    merge_to_natural[natural_to_merge] = np.arange(TOKENS, dtype=np.int32)
    edges_to_merge = np.full(2 * EDGE, -1, np.int32)
    for edge, merge in edge_to_half.items():
        edges_to_merge[edge] = merge + 72
        edges_to_merge[EDGE + edge] = merge
    return natural_to_merge, merge_to_natural, half_to_edge, source_to_window, window_to_source, edges_to_merge


N2M, M2N, H2E, S2W, W2S, E2M = token_tables()


def lanes(table):
    return jnp.asarray(table.reshape(1, -1))


def picks(rows, table):
    spots = lax.broadcasted_iota(jnp.int32, (rows, table.shape[1]), 0)
    return (spots == table).astype(F32).astype(BF16)


def mm(a, b):
    return jnp.dot(a, b, preferred_element_type=F32)


def mm_nt(a, b):
    return lax.dot_general(a, b, (((1,), (1,)), ((), ())), preferred_element_type=F32)


def mm_tn(a, b):
    return lax.dot_general(a, b, (((0,), (0,)), ((), ())), preferred_element_type=F32)


def normed_rows(values, gain):
    center = values - jnp.mean(values, axis=-1, keepdims=True)
    spread = jnp.mean(center * center, axis=-1, keepdims=True)
    return center * lax.rsqrt(spread + EPSILON) * gain


def front_kernel(
    fin, ids, level_table, surface_table, gain, n2m, h2e,
    fields_out, up_out, lo_out, lon_out, diag_out, table,
):
    table[...] = jnp.zeros_like(table)
    table[0:13, :] = level_table[...].astype(F32)
    table[13:15, :] = surface_table[...].astype(F32)
    order = picks(TOKENS, n2m[...])
    spots = lax.broadcasted_iota(jnp.int32, (16, TOKENS), 0)
    hot = ((spots == ids[0:1, :]) | (spots == ids[1:2, :])).astype(F32).astype(BF16)
    fields = mm(order, fin[...]) + mm(mm_nt(order, hot).astype(BF16), table[...].astype(BF16))
    fields_out[...] = fields
    normed = normed_rows(fields, gain[...].astype(F32).reshape(1, C1))
    up = jnp.concatenate([normed[q * COARSE : q * COARSE + 72] for q in range(4)], axis=0).astype(BF16)
    lo = jnp.concatenate([normed[q * COARSE + 72 : (q + 1) * COARSE] for q in range(4)], axis=0).astype(BF16)
    up_out[...] = up
    lo_out[...] = lo
    edge = picks(EDGE, h2e[...])
    lon_out[...] = mm(edge, lo).astype(BF16)
    diag_out[...] = mm(edge, up).astype(BF16)


def attention_kernel(flag, lo, up, lon, diag, w_qkv, s2w, w2s, lo_out, up_out, lon_out, diag_out, src, qkv, att):
    src[0:HALF, :] = lo[...]
    src[HALF : 2 * HALF, :] = up[...]
    src[2 * HALF : 2 * HALF + EDGE, :] = lon[...]
    src[2 * HALF + EDGE :, :] = diag[...]
    windows = mm(picks(TOKENS, s2w[...]), src[...]).astype(BF16)
    qkv[...] = mm(windows, w_qkv[...]).astype(BF16)
    size = 144
    top = lax.broadcasted_iota(jnp.int32, (size, size), 0)
    left = lax.broadcasted_iota(jnp.int32, (size, size), 1)

    def low(t):
        return ((t >= 36) & (t < 72)) | (t >= 108)

    apart = (low(top) != low(left)) & (flag[0] == 1)
    lane = lax.broadcasted_iota(jnp.int32, (size, 128), 1)
    first = lane < 64
    ones = [jnp.where(first, 1.0, 0.0).astype(BF16), jnp.where(first, 0.0, 1.0).astype(BF16)]

    def one_window(w, carry):
        rows = pl.ds(pl.multiple_of(w * size, 16), size)
        for pair in range(4):
            cols = pair * 128
            queries = qkv[rows, cols : cols + 128]
            keys = qkv[rows, C1 + cols : C1 + cols + 128]
            values = qkv[rows, 2 * C1 + cols : 2 * C1 + cols + 128]
            total = None
            for side in range(2):
                scores = mm_nt(queries * ones[side], keys) * (1.0 / math.sqrt(64))
                scores = jnp.where(apart, -1e30, scores)
                peak = jnp.max(scores, axis=-1, keepdims=True)
                probs = jnp.exp(scores - peak).astype(BF16)
                both = mm(probs, jnp.concatenate([values * ones[side], ones[side]], axis=1))
                total = both if total is None else total + both
            att[rows, cols : cols + 128] = (total[:, :128] / total[:, 128:]).astype(BF16)
        return carry

    lax.fori_loop(0, 4, one_window, 0)
    back = mm(picks(2 * HALF + 2 * EDGE, w2s[...]), att[...]).astype(BF16)
    lo_out[...] = back[0:HALF]
    up_out[...] = back[HALF : 2 * HALF]
    lon_out[...] = back[2 * HALF : 2 * HALF + EDGE]
    diag_out[...] = back[2 * HALF + EDGE :]


def merge_kernel(
    lo, up, lon, diag, fields, w_proj, merge_gain, w_merge, coarse_gain, e2m, skip_out, coarse_out, cn_out
):
    upper, lower = up[...].astype(F32), lo[...].astype(F32)
    parts = []
    for q in range(4):
        parts.append(upper[q * 72 : (q + 1) * 72])
        parts.append(lower[q * 72 : (q + 1) * 72])
    edges = jnp.concatenate([lon[...], diag[...]], axis=0)
    attended = (jnp.concatenate(parts, axis=0) + mm(picks(TOKENS, e2m[...]), edges)).astype(BF16)
    skip = (fields[...] + mm(attended, w_proj[...])).astype(BF16)
    skip_out[...] = skip
    skip = skip.astype(F32)
    blocks = [skip[q * COARSE : (q + 1) * COARSE] for q in range(4)]
    mean = sum(jnp.sum(b, axis=-1, keepdims=True) for b in blocks) * (1.0 / (4 * C1))
    blocks = [b - mean for b in blocks]
    spread = sum(jnp.sum(b * b, axis=-1, keepdims=True) for b in blocks) * (1.0 / (4 * C1))
    scale = lax.rsqrt(spread + EPSILON)
    coarse = None
    for q in range(4):
        gain = merge_gain[0:1, q * C1 : (q + 1) * C1].astype(F32)
        part = mm((blocks[q] * scale * gain).astype(BF16), w_merge[q * C1 : (q + 1) * C1, :])
        coarse = part if coarse is None else coarse + part
    coarse = coarse.astype(BF16)
    coarse_out[...] = coarse
    cn_out[...] = normed_rows(coarse.astype(F32), coarse_gain[...].astype(F32)).astype(BF16)


def quarter(source, held, sems, q):
    cols = pl.ds(pl.multiple_of(q * C1, C1), C1)
    return pltpu.make_async_copy(source.at[:, cols], held.at[:, cols], sems.at[q])


def cotangent_kernel(cot, n2m, w_expand, dc_out, ordered, total, held, sems):
    for q in range(4):
        quarter(w_expand, held, sems, q).start()
    ordered[...] = mm(picks(TOKENS, n2m[...]), cot[...]).astype(BF16)
    total[...] = jnp.zeros_like(total)

    def one_place(q, carry):
        quarter(w_expand, held, sems, q).wait()
        rows = pl.ds(pl.multiple_of(q * COARSE, 16), COARSE)
        cols = pl.ds(pl.multiple_of(q * C1, C1), C1)
        total[...] += mm_nt(ordered[rows, :], held[:, cols])
        return carry

    lax.fori_loop(0, 4, one_place, 0)
    dc_out[...] = total[...].astype(BF16)


NEAR = 80
QUAD = 4 * COARSE


def stack_into(full, refs):
    at = 0
    for ref in refs:
        full[at : at + ref.shape[0], :] = ref[...]
        at += ref.shape[0]


def hidden_rows(full, w_in, w_in_far, w_out, w_out_far, hidden_out, slope_out, partial):
    root = math.sqrt(2.0 / math.pi)

    def one_part(k, carry):
        rows = pl.ds(pl.multiple_of(k * (QUAD // 2), 32), QUAD // 2)
        total = None
        for side, (win, wout) in enumerate(((w_in, w_out), (w_in_far, w_out_far))):
            x = mm(full[rows, :], win[...])
            t = jnp.tanh(root * (x + 0.044715 * (x * x * x)))
            half = 0.5 * (1.0 + t)
            hidden = (x * half).astype(BF16)
            slope = half + 0.5 * x * (1.0 - t * t) * (root * (1.0 + 3 * 0.044715 * (x * x)))
            cols = slice(side * FB, (side + 1) * FB)
            hidden_out[rows, cols] = hidden
            slope_out[rows, cols] = slope.astype(BF16)
            part = mm(hidden, wout[...])
            total = part if total is None else total + part
        partial[rows, :] = total.astype(BF16)
        return carry

    lax.fori_loop(0, 2, one_part, 0)


def near_kernel(own, far, right, left, w_in, w_in_far, w_out, w_out_far, partial, full, hidden, slope):
    stack_into(full, (own, far, right, left))
    hidden_rows(full, w_in, w_in_far, w_out, w_out_far, hidden, slope, partial)


def wide_kernel(
    right, left, far_right2, far_left2, w_in, w_in_far, w_out, w_out_far,
    sides, send_right, send_left, full, hidden, slope, partial,
):
    full[0:NEAR, :] = right[0:NEAR, :]
    full[NEAR:COARSE, :] = left[0 : COARSE - NEAR, :]
    full[COARSE : 2 * COARSE, :] = right[NEAR:, :]
    full[2 * COARSE : 3 * COARSE, :] = left[COARSE - NEAR :, :]
    full[3 * COARSE : 3 * COARSE + NEAR, :] = far_right2[...]
    full[3 * COARSE + NEAR :, :] = far_left2[...]
    hidden_rows(full, w_in, w_in_far, w_out, w_out_far, hidden, slope, partial)
    sides[...] = partial[COARSE : 3 * COARSE, :]
    send_right[0:NEAR, :] = partial[0:NEAR, :]
    send_right[NEAR:, :] = partial[3 * COARSE : 3 * COARSE + NEAR, :]
    send_left[0 : COARSE - NEAR, :] = partial[NEAR:COARSE, :]
    send_left[COARSE - NEAR :, :] = partial[3 * COARSE + NEAR :, :]


def added(x, y):
    return (x.astype(F32) + y.astype(F32)).astype(BF16)


def pass_kernel(near, sides, got_right, got_left, own_r, own_l, far_r, far_l):
    rest = COARSE - NEAR
    far_left, far_right = sides[0:COARSE, :], sides[COARSE:, :]
    own_r[0:NEAR, :] = added(near[3 * COARSE : 3 * COARSE + NEAR, :], got_right[0:NEAR, :])
    own_r[NEAR:, :] = near[3 * COARSE + NEAR :, :]
    own_l[0:NEAR, :] = near[2 * COARSE : 2 * COARSE + NEAR, :]
    own_l[NEAR:, :] = added(near[2 * COARSE + NEAR : 3 * COARSE, :], got_left[0:rest, :])
    far_r[0:NEAR, :] = added(far_right[0:NEAR], got_right[NEAR:, :])
    far_r[NEAR:, :] = far_right[NEAR:]
    far_l[0:NEAR, :] = far_left[0:NEAR]
    far_l[NEAR:, :] = added(far_left[NEAR:], got_left[rest:, :])


def far_kernel(near, got_right, got_left, send):
    total = near[COARSE : 2 * COARSE, :].astype(F32) + got_right[...].astype(F32)
    send[...] = (total + got_left[...].astype(F32)).astype(BF16)


def gradient_kernel(
    own, far, right, left, right2, left2, far_rows, near_full, near_hidden, near_slope,
    wide_full, wide_hidden, wide_slope, w_out, w_out_far, own_sums, far_sums, dfull, dact,
):
    stack_into(dfull, (own, far, right, left, right2, left2, far_rows))
    for side, wout in enumerate((w_out, w_out_far)):
        cols = slice(side * FB, (side + 1) * FB)
        for part, slope in enumerate((near_slope, wide_slope)):
            rows = slice(part * QUAD, (part + 1) * QUAD)
            back = mm_nt(dfull[rows, :], wout[...])
            dact[rows, cols] = (back * slope[:, cols].astype(F32)).astype(BF16)

    def one_block(k, carry):
        c = pl.ds(pl.multiple_of(k * 256, 256), 256)
        out = mm_tn(dfull[0:QUAD, c], near_hidden[...]) + mm_tn(dfull[QUAD:, c], wide_hidden[...])
        into = mm_tn(near_full[:, c], dact[0:QUAD, :]) + mm_tn(wide_full[:, c], dact[QUAD:, :])
        for g, both in enumerate((out, into)):
            both = both.astype(BF16)
            for i in range(4):
                rows = pl.ds(pl.multiple_of(k * 512 + i * 128 + g * 64, 64), 64)
                own_sums[rows, :] = both[i * 64 : (i + 1) * 64, :FB]
                far_sums[rows, :] = both[i * 64 : (i + 1) * 64, FB:]
        return carry

    lax.fori_loop(0, 4, one_block, 0)


def pair_kernel(side, own, got, mine, other):
    for out, half in ((mine, side[0]), (other, 1 - side[0])):
        rows = pl.ds(pl.multiple_of(half * C2, C2), C2)
        out[...] = added(own[rows, :], got[rows, :])


def expand_kernel(coarse, near, got_right, got_left, got_far, skip, m2n, w_expand, fields_out, parts, held, sems):
    for q in range(4):
        quarter(w_expand, held, sems, q).start()
    mixed = near[0:COARSE, :].astype(F32) + got_right[...].astype(F32)
    mixed = mixed + (got_left[...].astype(F32) + got_far[...].astype(F32))
    coarse_out = (coarse[...].astype(F32) + mixed).astype(BF16)

    def one_place(q, carry):
        rows = pl.ds(pl.multiple_of(q * COARSE, 16), COARSE)
        cols = pl.ds(pl.multiple_of(q * C1, C1), C1)
        quarter(w_expand, held, sems, q).wait()
        parts[rows, :] = (skip[rows, :].astype(F32) + mm(coarse_out, held[:, cols])).astype(BF16)
        return carry

    lax.fori_loop(0, 4, one_place, 0)
    fields_out[...] = mm(picks(TOKENS, m2n[...]), parts[...]).astype(BF16)


def shaped(dims, dtype=BF16):
    return jax.ShapeDtypeStruct(dims, dtype)


FETCH = (pltpu.VMEM((C2, 4 * C1), BF16), pltpu.SemaphoreType.DMA((4,)))


def run(kernel, outs, args, flops, scratch=(), smem=(), hbm=(), vmem=20):
    nbytes = sum(a.size * a.dtype.itemsize for a in args) + sum(math.prod(o.shape) * 2 for o in outs)
    spaces = [pltpu.SMEM if k in smem else pl.ANY if k in hbm else pltpu.VMEM for k in range(len(args))]
    return pl.pallas_call(
        kernel,
        out_shape=tuple(outs),
        in_specs=[pl.BlockSpec(memory_space=space) for space in spaces],
        out_specs=tuple(pl.BlockSpec(memory_space=pltpu.VMEM) for _ in outs),
        scratch_shapes=list(scratch),
        compiler_params=pltpu.CompilerParams(vmem_limit_bytes=vmem and vmem * 1024 * 1024),
        cost_estimate=pl.CostEstimate(flops=int(flops), bytes_accessed=int(nbytes), transcendentals=0),
    )(*args)


def lat_of(y, x, core):
    return (y % 2) * 8 + (x % 4) * 2 + core % 2


def lat_moves(dy, dx, dcore):
    return [(l, lat_of(l // 8 + dy, l // 2 % 4 + dx, l % 2 + dcore)) for l in range(16)]


def on_lat(value, dy=0, dx=0, dcore=0):
    return lax.ppermute(value, "lat", lat_moves(dy, dx, dcore))


def shift(value, axes, steps):
    if axes == "both":
        pairs = [
            (o * 16 + l, (o + steps) % 16 * 16 + (l + steps) % 16) for o in range(16) for l in range(16)
        ]
        return lax.ppermute(value, ("lon", "lat"), pairs)
    return lax.ppermute(value, axes, [(s, (s + steps) % 16) for s in range(16)])


def gathered(block):
    far = on_lat(block, dy=1)
    right, left = on_lat(block, dx=1), on_lat(block, dx=-1)
    right2 = on_lat(jnp.concatenate([right[:NEAR], far], axis=0), dx=1)
    left2 = on_lat(jnp.concatenate([left[NEAR:], far], axis=0), dx=-1)
    far_right2, far_left2 = on_lat(right2[NEAR : 2 * NEAR], dx=1), on_lat(left2[COARSE:], dx=-1)
    return (block, far, right, left), (right2, left2, far_right2, far_left2)


def gathered_behind(block):
    far = on_lat(block, dy=1)
    right, left = on_lat(block, dx=1), on_lat(block, dx=-1)
    right2, left2 = on_lat(right[:NEAR], dx=1), on_lat(left[NEAR:], dx=-1)
    far_rows = on_lat(jnp.concatenate([right, left, right2, left2], axis=0), dy=1)
    return block, far, right, left, right2, left2, far_rows


EIGHTS = [[half * 8 + z for z in range(8)] for half in range(2)]


def whole(
    fields_in, level_map, land_sea, level_table, surface_table, norm_gain, w_qkv, w_proj, merge_gain,
    w_merge, coarse_gain, w_in, w_out, w_expand, cotangent,
):
    lat, lon_index = lax.axis_index("lat"), lax.axis_index("lon")
    surface = 13 + (land_sea == 1).astype(jnp.int32)
    ids = jnp.concatenate([level_map.reshape(2 * ROWS, COLS), surface, surface], axis=0).reshape(2, TOKENS)
    w_in_far, w_out_far = on_lat(w_in, dcore=1), on_lat(w_out, dcore=1)
    fields, up, lo, lon, diag = run(
        front_kernel,
        [shaped((TOKENS, C1), F32), shaped((HALF, C1)), shaped((HALF, C1)), shaped((EDGE, C1)), shaped((EDGE, C1))],
        (
            fields_in.reshape(TOKENS, C1), ids,
            level_table, surface_table, norm_gain, lanes(N2M), lanes(H2E),
        ),
        4e8,
        [pltpu.VMEM((16, C1), F32)],
        vmem=None,
    )
    up, lon, diag = shift(up, "lat", -1), shift(lon, "lon", -1), shift(diag, "both", -1)
    (dc,) = run(
        cotangent_kernel, [shaped((COARSE, C2))], (cotangent.reshape(TOKENS, C1), lanes(N2M), w_expand), 1e9,
        [pltpu.VMEM((TOKENS, C1), BF16), pltpu.VMEM((COARSE, C2), F32), *FETCH], hbm=(2,), vmem=None,
    )
    dc_pieces = gathered_behind(dc)
    flag = (lat == 15).astype(jnp.int32).reshape(1)
    lo, up, lon, diag = run(
        attention_kernel,
        [shaped((HALF, C1)), shaped((HALF, C1)), shaped((EDGE, C1)), shaped((EDGE, C1))],
        (flag, lo, up, lon, diag, w_qkv, lanes(S2W), lanes(W2S)),
        3e9,
        [pltpu.VMEM((2 * HALF + 2 * EDGE, C1), BF16), pltpu.VMEM((TOKENS, 3 * C1), BF16), pltpu.VMEM((TOKENS, C1), BF16)],
        smem=(0,),
    )
    up, lon, diag = shift(up, "lat", 1), shift(lon, "lon", 1), shift(diag, "both", 1)
    skip, coarse, cn = run(
        merge_kernel,
        [shaped((TOKENS, C1)), shaped((COARSE, C2)), shaped((COARSE, C2))],
        (lo, up, lon, diag, fields, w_proj, merge_gain.reshape(1, 4 * C1), w_merge, coarse_gain.reshape(1, C2), lanes(E2M)),
        2e9,
    )
    cn_near, cn_wide = gathered(cn)
    weights = (w_in, w_in_far, w_out, w_out_far)
    kept = [shaped((QUAD, C2)), shaped((QUAD, 2 * FB)), shaped((QUAD, 2 * FB))]
    near, *near_kept = run(near_kernel, [shaped((QUAD, C2)), *kept], (*cn_near, *weights), 2.5e9)
    sides, to_right, to_left, *wide_kept = run(
        wide_kernel,
        [shaped((2 * COARSE, C2)), shaped((2 * NEAR, C2)), shaped((2 * (COARSE - NEAR), C2)), *kept],
        (*cn_wide, *weights),
        2.5e9,
        [pltpu.VMEM((QUAD, C2), BF16)],
    )
    got_right, got_left = on_lat(to_right, dx=1), on_lat(to_left, dx=-1)
    own_sums, far_sums = run(
        gradient_kernel,
        [shaped((2 * C2, FB))] * 2,
        (*dc_pieces, *near_kept, *wide_kept, w_out, w_out_far),
        4e9,
        [pltpu.VMEM((8 * COARSE, C2), BF16), pltpu.VMEM((8 * COARSE, 2 * FB), BF16)],
    )
    own_r, own_l, far_r, far_l = run(pass_kernel, [shaped((COARSE, C2))] * 4, (near, sides, got_right, got_left), 1e8)
    far_r, far_l = on_lat(far_r, dx=1), on_lat(far_l, dx=-1)
    own_r, own_l = on_lat(own_r, dx=1), on_lat(own_l, dx=-1)
    (across,) = run(far_kernel, [shaped((COARSE, C2))], (near, far_r, far_l), 1e8)
    across = on_lat(across, dy=1)

    got_sums = on_lat(far_sums, dcore=1)
    side = (lon_index // 8).astype(jnp.int32).reshape(1)
    mine, other = run(pair_kernel, [shaped((C2, FB))] * 2, (side, own_sums, got_sums), 1e8, smem=(0,))
    other = lax.ppermute(other, "lon", [(o, (o + 8) % 16) for o in range(16)])
    both = added(mine, other).reshape(8, 128, FB)
    pieces = lax.all_to_all(both, "lon", 0, 0, axis_index_groups=EIGHTS, tiled=True)
    total = jnp.sum(pieces.astype(F32), axis=0)
    grad_out, grad_in = total[:64].T, total[64:]
    (fields_out,) = run(
        expand_kernel,
        [shaped((TOKENS, C1))],
        (coarse, near, own_r, own_l, across, skip, lanes(M2N), w_expand),
        1e9,
        [pltpu.VMEM((TOKENS, C1), BF16), *FETCH],
        hbm=(7,),
        vmem=None,
    )
    return (fields_out.reshape(LEVELS, ROWS, COLS, C1), grad_in, grad_out)


def solution(mesh):
    placed = (
        P(None, "lat", "lon", None),
        P(None, "lat", "lon"),
        P("lat", "lon"),
        P(),
        P(),
        P(),
        P(),
        P(),
        P(),
        P(),
        P(),
        P(None, "lat"),
        P("lat", None),
        P(),
        P(None, "lat", "lon", None),
    )
    return jax.shard_map(
        whole,
        mesh=mesh,
        in_specs=placed,
        out_specs=(P(None, "lat", "lon", None), P("lon", "lat"), P("lat", "lon")),
        check_vma=False,
    )
```
